32 devices in a mesh: row: 16 (over z, y, x), col: 2 (over core).
Axes of the slice: x: 2, y: 2, z: 4, core: 2. Of those that a mesh axis runs over, the one named last changes fastest.
Arguments:
- incident: bfloat16 [2, 8192, 512], P(None, ('row', 'col')), may hold values from -6 to 6
- near_tiles: bfloat16 [32, 2, 3, 2, 256, 256], P(('row', 'col')), may hold values from -0.15625 to 0.15625
- near_offsets: int32 [32, 3], P(('row', 'col')), may hold values from -2 to 2, as said below
- far_row: int32 [16, 2, 16], P('row', 'col'), may hold values from 0 to 1, as said below
- far_col: int32 [16, 2, 16], P('row', 'col'), may hold values from 0 to 15
- far_rank: int32 [16, 2, 16], P('row', 'col'), may hold values from 8 to 32, as said below
- far_count: int32 [16, 2], P('row', 'col'), may hold values from 2 to 16, as said below
- far_u: bfloat16 [16, 2, 2, 16, 2, 32, 256], P('row', 'col'), may hold values from -0.25 to 0.25
- far_v: bfloat16 [16, 2, 2, 16, 2, 32, 256], P('row', 'col'), may hold values from -0.25 to 0.25
Outputs:
- response: bfloat16 [2, 8192, 512], P(None, ('row', 'col'))
The draws below stay inside these ranges and needn't reach their ends.
Inputs may be any that keep to these rules, and one draw needn't show every extreme that they name: `near_offsets`: slot 0 of every tile is 0; the other slots of a tile hold distinct values among -2, -1, 1, 2. On one device the pairs (far_row, far_col) of all 16 slots are distinct, and every block (i, j) they name has circular tile distance 3 or more between i and j. `far_rank`: slot 0 of every device has rank 32. `far_count`: some device has all 16 slots live.
All inputs are finite; a program needn't handle non-finite values.
Results may differ from the reference program's by a relative error of at most 0.0035.
Values may be sent and summed in bfloat16 or wider, within the bound.
A program may use at most 192 MiB of HBM per device.

```python
import jax
import jax.numpy as jnp
from jax import lax

TILE = 256
RANK = 32
NEAR_SLOTS = 3
WAVES = 2
SOURCES = 256
FAR_SLOTS = 16
TILES = 32
PANELS = 8192
N_ROW = 16
N_COL = 2


def draw_near_offsets(key, part):
    tile_count = N_ROW * N_COL
    scores = jax.random.randint(jax.random.fold_in(key, 11), (tile_count, 4), 0, 1 << 20) * 4 + jnp.arange(4, dtype=jnp.int32)[None, :]
    ranking = jnp.argsort(scores, axis=1)
    offset_table = jnp.array([-2, -1, 1, 2], dtype=jnp.int32)
    picked = offset_table[ranking[:, :NEAR_SLOTS - 1]]
    return jnp.concatenate([jnp.zeros((tile_count, 1), jnp.int32), picked], axis=1).astype(jnp.int32)


def far_layout(key):
    pair_count = N_COL * N_ROW
    tile_count = N_ROW * N_COL
    pair_ids = jnp.arange(pair_count, dtype=jnp.int32)
    local_row = pair_ids // N_ROW
    col_device = pair_ids % N_ROW
    row_index = jnp.arange(N_ROW, dtype=jnp.int32)[:, None, None]
    col_index = jnp.arange(N_COL, dtype=jnp.int32)[None, :, None]
    row_tile = row_index * N_COL + local_row[None, None, :]
    col_tile = col_device[None, None, :] * N_COL + col_index
    forward_gap = (row_tile - col_tile) % tile_count
    circular = jnp.minimum(forward_gap, tile_count - forward_gap)
    random_part = jax.random.randint(jax.random.fold_in(key, 21), (N_ROW, N_COL, pair_count), 0, 1 << 19)
    scores = random_part * 1024 + pair_ids[None, None, :] + jnp.where(circular < 3, 1 << 30, 0)
    ranking = jnp.argsort(scores, axis=2)[:, :, :FAR_SLOTS]
    return ((ranking // N_ROW).astype(jnp.int32), (ranking % N_ROW).astype(jnp.int32))


def draw_far_row(key, part):
    return far_layout(key)[0]


def draw_far_col(key, part):
    return far_layout(key)[1]


def draw_far_rank(key, part):
    sampled = jax.random.randint(jax.random.fold_in(key, 31), (N_ROW, N_COL, FAR_SLOTS), max(1, RANK // 4), RANK + 1)
    leading = (jnp.arange(FAR_SLOTS, dtype=jnp.int32) == 0)[None, None, :]
    return jnp.where(leading, RANK, sampled).astype(jnp.int32)


def draw_far_count(key, part):
    lowest = max(1, FAR_SLOTS // 8)
    spread = FAR_SLOTS - lowest
    uniform_part = jax.random.randint(jax.random.fold_in(key, 41), (N_ROW, N_COL), 0, spread + 1)
    counts = lowest + uniform_part * uniform_part // spread
    fullest = jax.random.randint(jax.random.fold_in(key, 42), (), 0, N_ROW * N_COL)
    flat_index = jnp.arange(N_ROW * N_COL, dtype=jnp.int32).reshape(N_ROW, N_COL)
    return jnp.where(flat_index == fullest, FAR_SLOTS, counts).astype(jnp.int32)


def levels(rng, extent, pieces, least, high):
    def one(position, parts):
        draws = jax.random.uniform(jax.random.fold_in(jax.random.fold_in(rng, 6), position), (parts,), jnp.float32, least / len(pieces), high / len(pieces))
        return jnp.repeat(jnp.exp(draws), extent[position] // parts).reshape((-1,) + (1,) * (len(extent) - position - 1))

    loudness = one(*pieces[0])
    for cut in pieces[1:]:
        loudness = loudness * one(*cut)
    return loudness


def normal_values(own_key, extent, width, most, pieces=(), held_as=jnp.bfloat16):
    level = levels(own_key, extent, pieces, -0.22, 0.18) if pieces else 1.0
    drawn = jax.random.normal(own_key, extent, jnp.float32) * width * level
    return jnp.minimum(jnp.maximum(drawn, -most), most).astype(held_as)


def setup_inputs(seed: int = 0) -> dict:
    keys = jax.random.split(jax.random.key(seed), 10)
    return {
        "incident": normal_values(keys[0], (WAVES, PANELS, 2 * SOURCES), 1.0, 6.0, ((1, 32),)),
        "near_tiles": normal_values(keys[1], (TILES, WAVES, NEAR_SLOTS, 2, TILE, TILE), (2 * TILE * NEAR_SLOTS) ** -0.5, 0.15625, ((0, 32),)),
        "near_offsets": draw_near_offsets(jax.random.fold_in(keys[9], 71), 0),
        "far_row": draw_far_row(jax.random.fold_in(keys[9], 71), 0),
        "far_col": draw_far_col(jax.random.fold_in(keys[9], 71), 0),
        "far_rank": draw_far_rank(jax.random.fold_in(keys[9], 71), 0),
        "far_count": draw_far_count(jax.random.fold_in(keys[9], 71), 0),
        "far_u": normal_values(keys[7], (N_ROW, N_COL, WAVES, FAR_SLOTS, 2, RANK, TILE), (RANK * FAR_SLOTS) ** -0.5, 0.25, ((0, 16), (1, 2))),
        "far_v": normal_values(keys[8], (N_ROW, N_COL, WAVES, FAR_SLOTS, 2, RANK, TILE), (2 * TILE) ** -0.5, 0.25, ((0, 16), (1, 2))),
    }


def combine_parts(real_prod, imag_prod):
    half_width = real_prod.shape[-1] // 2
    return jnp.concatenate([real_prod[..., :half_width] - imag_prod[..., half_width:], real_prod[..., half_width:] + imag_prod[..., :half_width]], axis=-1)


def reference(incident, near_tiles, near_offsets, far_row, far_col, far_rank, far_count, far_u, far_v):
    tile_count = N_ROW * N_COL
    columns = incident.shape[-1]
    tiles_input = incident.reshape(WAVES, tile_count, TILE, columns)
    near_groups = near_tiles.reshape(N_ROW, N_COL, WAVES, NEAR_SLOTS, 2, TILE, TILE)
    offset_groups = near_offsets.reshape(N_ROW, N_COL, NEAR_SLOTS)
    slot_ids = jnp.arange(FAR_SLOTS, dtype=jnp.int32)
    rank_ids = jnp.arange(RANK, dtype=jnp.int32)
    block_ids = jnp.arange(N_COL, dtype=jnp.int32)

    def one_group(packed):
        group_index, near_part, offset_part, rows_part, cols_part, rank_part, count_part, u_part, v_part = packed
        own_tiles = group_index * N_COL + block_ids
        near_index = ((own_tiles[:, None] + offset_part) % tile_count).astype(jnp.int32)
        near_inputs = tiles_input[:, near_index].astype(jnp.float32)
        near_float = near_part.astype(jnp.float32)
        real_prod = jnp.einsum("awnpq,wanqc->wapc", near_float[:, :, :, 0], near_inputs)
        imag_prod = jnp.einsum("awnpq,wanqc->wapc", near_float[:, :, :, 1], near_inputs)
        result_rows = combine_parts(real_prod, imag_prod)
        for col_group in range(N_COL):
            col_tiles = (cols_part[col_group] * N_COL + col_group).astype(jnp.int32)
            live_mask = ((slot_ids < count_part[col_group])[:, None] & (rank_ids[None, :] < rank_part[col_group][:, None])).astype(jnp.float32)
            select = (rows_part[col_group][:, None] == block_ids[None, :]).astype(jnp.float32)
            for wave_index in range(WAVES):
                slot_tiles = tiles_input[wave_index, col_tiles].astype(jnp.float32)
                v_factor = v_part[col_group, wave_index].astype(jnp.float32)
                coefficients = combine_parts(jnp.einsum("fkq,fqc->fkc", v_factor[:, 0], slot_tiles), jnp.einsum("fkq,fqc->fkc", v_factor[:, 1], slot_tiles))
                coefficients = lax.optimization_barrier((coefficients * live_mask[:, :, None]).astype(jnp.bfloat16)).astype(jnp.float32)
                u_factor = u_part[col_group, wave_index].astype(jnp.float32)
                contrib = combine_parts(jnp.einsum("fkp,fkc->fpc", u_factor[:, 0], coefficients), jnp.einsum("fkp,fkc->fpc", u_factor[:, 1], coefficients))
                added = jnp.einsum("fa,fpc->apc", select, contrib, precision=lax.Precision.HIGHEST)
                result_rows = result_rows.at[wave_index].add(added)
        return result_rows.astype(jnp.bfloat16)

    grouped = lax.map(one_group, (jnp.arange(N_ROW, dtype=jnp.int32), near_groups, offset_groups, far_row, far_col, far_rank, far_count, far_u, far_v))
    return jnp.transpose(grouped, (1, 0, 2, 3, 4)).reshape(WAVES, tile_count * TILE, columns)
```

```python
import functools

import jax
import jax.numpy as jnp
from jax import lax
from jax.experimental import pallas as pl
from jax.experimental.pallas import tpu as pltpu
from jax.sharding import PartitionSpec as P

MESH = pl.DeviceIdType.MESH
UP, DOWN, ALONG_Y, ALONG_X = range(4)


def from_behind(value, axis, steps):
    count = lax.axis_size(axis)
    pairs = [(source, (source + steps) % count) for source in range(count)]
    return lax.ppermute(value, axis, pairs)


def combine_parts(real_prod, imag_prod):
    half_width = real_prod.shape[-1] // 2
    return jnp.concatenate(
        [
            real_prod[..., :half_width] - imag_prod[..., half_width:],
            real_prod[..., half_width:] + imag_prod[..., :half_width],
        ],
        axis=-1,
    )


def far_partial(
    wave_tiles,
    rows_local,
    cols_local,
    rank_local,
    live_count,
    u_wave,
    v_wave,
    group_limit,
    row_blocks,
):
    group_size = 16
    tile_rows = wave_tiles.shape[1]
    columns = wave_tiles.shape[2]
    rank_size = v_wave.shape[2]
    slot_ids = jnp.arange(group_size, dtype=jnp.int32)
    rank_ids = jnp.arange(rank_size, dtype=jnp.int32)

    def add_group(group_step, far_sum):
        first_slot = group_step * group_size
        rows_group = lax.dynamic_slice_in_dim(rows_local, first_slot, group_size)
        cols_group = lax.dynamic_slice_in_dim(cols_local, first_slot, group_size)
        rank_group = lax.dynamic_slice_in_dim(rank_local, first_slot, group_size)
        v_group = lax.dynamic_slice_in_dim(v_wave, first_slot, group_size, 0)
        u_group = lax.dynamic_slice_in_dim(u_wave, first_slot, group_size, 0)
        slot_tiles = jnp.take(wave_tiles, cols_group, axis=0)
        real_prod = jnp.einsum(
            "fkq,fqc->fkc", v_group[:, 0], slot_tiles, preferred_element_type=jnp.float32
        )
        imag_prod = jnp.einsum(
            "fkq,fqc->fkc", v_group[:, 1], slot_tiles, preferred_element_type=jnp.float32
        )
        live_mask = (first_slot + slot_ids < live_count)[:, None] & (
            rank_ids[None, :] < rank_group[:, None]
        )
        coefficients = (
            combine_parts(real_prod, imag_prod) * live_mask[:, :, None].astype(jnp.float32)
        ).astype(jnp.bfloat16)
        real_back = jnp.einsum(
            "fkp,fkc->fpc", u_group[:, 0], coefficients, preferred_element_type=jnp.float32
        )
        imag_back = jnp.einsum(
            "fkp,fkc->fpc", u_group[:, 1], coefficients, preferred_element_type=jnp.float32
        )
        contrib = combine_parts(real_back, imag_back)
        return far_sum.at[rows_group].add(contrib)

    zero_sum = jnp.zeros((row_blocks, tile_rows, columns), jnp.float32)
    return lax.fori_loop(0, group_limit, add_group, zero_sum)


def reduce_rows(far_sum, row_blocks, tile_rows, columns):
    flat_rows = far_sum.reshape(row_blocks * tile_rows, columns)
    return lax.psum_scatter(flat_rows, "col", scatter_dimension=0, tiled=True)


def generic_shards(incident, near_tiles, near_offsets, far_row, far_col, far_rank, far_count, far_u, far_v):
    wave_count, tile_rows, columns = incident.shape
    row_blocks = lax.axis_size("col")
    slot_count = far_row.shape[2]
    stacked = []
    for shift_by in (2, 1, 0, -1, -2):
        if shift_by == 0:
            stacked.append(incident)
        else:
            stacked.append(from_behind(incident, ("row", "col"), shift_by))
    neighbour = jnp.stack(stacked, axis=1)
    near_inputs = jnp.take(neighbour, near_offsets[0] + 2, axis=1)
    local_near = near_tiles[0]
    real_prod = jnp.einsum(
        "wnpq,wnqc->wpc", local_near[:, :, 0], near_inputs, preferred_element_type=jnp.float32
    )
    imag_prod = jnp.einsum(
        "wnpq,wnqc->wpc", local_near[:, :, 1], near_inputs, preferred_element_type=jnp.float32
    )
    near_total = combine_parts(real_prod, imag_prod)
    rows_local = far_row[0, 0]
    cols_local = far_col[0, 0]
    rank_local = far_rank[0, 0]
    live_count = far_count[0, 0]
    group_limit = slot_count // 16
    gathered = lax.all_gather(incident, "row", axis=1, tiled=True)
    outputs = []
    for wave_index in range(wave_count):
        wave_columns = gathered[wave_index]
        wave_tiles = wave_columns.reshape(-1, tile_rows, columns)
        far_sum = far_partial(
            wave_tiles,
            rows_local,
            cols_local,
            rank_local,
            live_count,
            far_u[0, 0, wave_index],
            far_v[0, 0, wave_index],
            group_limit,
            row_blocks,
        )
        own_rows = reduce_rows(far_sum, row_blocks, tile_rows, columns)
        outputs.append(near_total[wave_index] + own_rows)
    return jnp.stack(outputs, axis=0).astype(jnp.bfloat16)


def turned(block):
    half = block.shape[-1] // 2
    return jnp.concatenate([-block[:, half:], block[:, :half]], axis=-1)


def fused_kernel(
    depth, slot_ref, offset_ref, x_ref, near_hbm, u_hbm, v_hbm, out_ref,
    tiles, near_buf, u_buf, v_buf, u_dense, coef, outgoing, incoming, total,
    recv_sem, send_sem, pair_sem, sum_send, sum_recv, load_sem,
):
    waves = x_ref.shape[0]
    row_count = depth * 4
    rank_rows = v_buf.shape[3]
    r = lax.axis_index("row")
    c = lax.axis_index("col")
    z, y, x = r // 4, (r // 2) % 2, r % 2
    own_slot, edge_slot = row_count, row_count + 1
    edge_tile = (r + 1 - 2 * c + row_count) % row_count

    def row_of(tz, ty, tx):
        return (tz * 2 + ty) * 2 + tx

    loads = [
        pltpu.make_async_copy(v_hbm.at[0, 0], v_buf, load_sem.at[0]),
        pltpu.make_async_copy(u_hbm.at[0, 0], u_buf, load_sem.at[1]),
        pltpu.make_async_copy(near_hbm.at[0], near_buf, load_sem.at[2]),
    ]
    for load in loads:
        load.start()

    barrier = pltpu.get_barrier_semaphore()
    greeted = (
        (row_of((z + 1) % depth, y, x), c),
        (row_of((z + depth - 1) % depth, y, x), c),
        (row_of(z, 1 - y, x), c),
        (row_of(z, y, 1 - x), c),
        (r, 1 - c),
    )
    for device in greeted:
        pl.semaphore_signal(barrier, inc=1, device_id=device, device_id_type=MESH)
    pl.semaphore_wait(barrier, len(greeted))

    def hop(wave, tile, link, source=None, step=None):
        if step is None:
            step = 1 if link == UP else -1
        target = {
            ALONG_Y: (z, 1 - y, x),
            ALONG_X: (z, y, 1 - x),
        }.get(link if isinstance(link, int) else None)
        if target is None:
            target = (jnp.minimum(jnp.maximum(z + step, 0), depth - 1), y, x)
        return pltpu.make_async_remote_copy(
            src_ref=tiles.at[wave, tile] if source is None else source,
            dst_ref=tiles.at[wave, tile],
            send_sem=send_sem.at[wave, tile, link],
            recv_sem=recv_sem.at[wave, tile],
            device_id=(row_of(*target), c),
            device_id_type=MESH,
        )

    def to_pair(wave, source, slot):
        return pltpu.make_async_remote_copy(
            src_ref=source,
            dst_ref=tiles.at[wave, slot],
            send_sem=pair_sem.at[wave, slot - row_count],
            recv_sem=recv_sem.at[wave, slot],
            device_id=(r, 1 - c),
            device_id_type=MESH,
        )

    def first_link(wave):
        return ALONG_Y if wave % 2 == 0 else ALONG_X

    def second_link(wave):
        return ALONG_X if wave % 2 == 0 else ALONG_Y

    def project(wave, tile):
        block = tiles[wave, tile]
        row_blocks = slot_ref.shape[1]
        factors = [
            v_buf[wave, slot_ref[0, a, tile]].reshape(2 * rank_rows, -1) for a in range(row_blocks)
        ]
        prod = jnp.dot(
            jnp.concatenate(factors, axis=0), block, preferred_element_type=jnp.float32
        )
        ids = lax.broadcasted_iota(jnp.int32, (rank_rows, block.shape[1]), 0)
        for a in range(row_blocks):
            at = 2 * rank_rows * a
            both = combine_parts(prod[at:at + rank_rows], prod[at + rank_rows:at + 2 * rank_rows])
            both = jnp.where(ids < slot_ref[1, a, tile], both, 0.0)
            coef[wave, a, 0, tile] = both.astype(jnp.bfloat16)
            coef[wave, a, 1, tile] = turned(both).astype(jnp.bfloat16)

    def arrive(wave, tile):
        pltpu.make_async_copy(tiles.at[wave, tile], tiles.at[wave, tile], recv_sem.at[wave, tile]).wait()

    def share_edge(wave, tile):
        @pl.when(tile == edge_tile)
        def _():
            to_pair(wave, tiles.at[wave, tile], edge_slot).start()

    for wave in range(waves):
        own = x_ref.at[wave]
        hop(wave, r, first_link(wave), own).start()

        @pl.when(z < depth - 1)
        def _():
            hop(wave, r, UP, own).start()

        @pl.when(z > 0)
        def _():
            hop(wave, r, DOWN, own).start()

    for wave in range(waves):
        own = x_ref.at[wave]
        hop(wave, r, second_link(wave), own).start()
        to_pair(wave, own, own_slot).start()
        tiles[wave, r] = x_ref[wave]
    for load in loads:
        load.wait()

    def place_u(tile, carry):
        for wave in range(waves):
            for a in range(slot_ref.shape[1]):
                factor = u_buf[wave, slot_ref[0, a, tile]]
                u_dense[wave, a, 0, tile] = factor[0]
                u_dense[wave, a, 1, tile] = factor[1]
        return carry

    lax.fori_loop(0, row_count, place_u, 0)
    for wave in range(waves):
        project(wave, r)

    level_count = 2 * depth - 1
    lag = 2

    def level_of(step):
        sign = 1 - 2 * (step % 2)
        return z + sign * ((step + 1) // 2), sign

    def inside(level):
        return (level >= 0) & (level < depth)

    def spread(step, carry):
        level, sign = level_of(step)

        @pl.when((step < level_count) & inside(level))
        def _():
            tile = row_of(level, y, x)
            for wave in range(waves):
                arrive(wave, tile)

                @pl.when(inside(z - sign))
                def _():
                    hop(wave, tile, (1 + sign) // 2, step=-sign).start()

                hop(wave, tile, first_link(wave)).start()
                hop(wave, tile, second_link(wave)).start()
                share_edge(wave, tile)
            for wave in range(waves):
                project(wave, tile)

        behind, _ = level_of(jnp.maximum(step - lag, 0))

        @pl.when((step >= lag) & inside(behind))
        def _():
            for wave in range(waves):
                tile = row_of(behind, 1 - y, x) if wave % 2 == 0 else row_of(behind, y, 1 - x)
                arrive(wave, tile)
                hop(wave, tile, second_link(wave)).start()
                share_edge(wave, tile)
                project(wave, tile)

        return carry

    lax.fori_loop(1, level_count + lag, spread, 0)

    def finish(step, carry):
        level, _ = level_of(step % level_count)
        far_corner = step // level_count

        @pl.when(inside(level))
        def _():
            for wave in range(waves):
                if wave % 2 == 0:
                    tile = row_of(level, y + far_corner * (1 - 2 * y), 1 - x)
                else:
                    tile = row_of(level, 1 - y, x + far_corner * (1 - 2 * x))
                arrive(wave, tile)
                share_edge(wave, tile)
                project(wave, tile)

        return carry

    lax.fori_loop(0, 2 * level_count, finish, 0)

    def far_sum(wave, a):
        left = u_dense[wave, a].reshape(-1, u_dense.shape[-1])
        right = coef[wave, a].reshape(-1, coef.shape[-1])
        return lax.dot_general(
            left, right, (((0,), (0,)), ((), ())), preferred_element_type=jnp.float32
        )

    def send_sum(wave):
        return pltpu.make_async_remote_copy(
            src_ref=outgoing.at[wave],
            dst_ref=incoming.at[wave],
            send_sem=sum_send.at[wave],
            recv_sem=sum_recv.at[wave],
            device_id=(r, 1 - c),
            device_id_type=MESH,
        )

    def fill(wave, carry):
        outgoing[wave] = far_sum(wave, 1 - c)
        return carry

    lax.fori_loop(0, waves, fill, 0)
    for wave in range(waves):
        arrive(wave, own_slot)
        arrive(wave, edge_slot)

    def place_of(offset):
        even = (r + offset // 2 + row_count) % row_count
        same_chip = offset == 1 - 2 * c
        return jnp.where(offset % 2 == 0, even, jnp.where(same_chip, own_slot, edge_slot))

    def own_rows(wave, carry):
        send_sum(wave).start()
        value = far_sum(wave, c)
        for n in range(near_buf.shape[1]):
            block = tiles[wave, place_of(offset_ref[n])]
            value += jnp.dot(near_buf[wave, n, 0], block, preferred_element_type=jnp.float32)
            value += jnp.dot(
                near_buf[wave, n, 1], turned(block), preferred_element_type=jnp.float32
            )
        total[wave] = value
        return carry

    lax.fori_loop(0, waves, own_rows, 0)
    for wave in range(waves):
        send_sum(wave).wait()
        out_ref[wave] = (total[wave] + incoming[wave]).astype(out_ref.dtype)

    for wave in range(waves):
        to_pair(wave, x_ref.at[wave], own_slot).wait_send()
        to_pair(wave, x_ref.at[wave], edge_slot).wait_send()

    def drain(level, carry):
        tile = row_of(level, y, x)
        for wave in range(waves):
            hop(wave, tile, ALONG_Y).wait_send()
            hop(wave, tile, ALONG_X).wait_send()

            @pl.when((level <= z) & (z < depth - 1))
            def _():
                hop(wave, tile, UP).wait_send()

            @pl.when((level >= z) & (z > 0))
            def _():
                hop(wave, tile, DOWN).wait_send()

            passed = row_of(level, 1 - y, x) if wave % 2 == 0 else row_of(level, y, 1 - x)
            hop(wave, passed, second_link(wave)).wait_send()
        return carry

    lax.fori_loop(0, depth, drain, 0)


def fused_shards(incident, near_tiles, near_offsets, far_row, far_col, far_rank, far_count, far_u, far_v):
    waves, tile_rows, columns = incident.shape
    row_count, row_blocks = lax.axis_size("row"), lax.axis_size("col")
    slots, rank_rows = far_u.shape[3], far_u.shape[5]
    near_slots = near_tiles.shape[2]
    slot_ids = jnp.arange(slots, dtype=jnp.int32)
    block_key = far_row[0, 0] * row_count + far_col[0, 0]
    live = slot_ids < far_count[0, 0]
    match = (block_key[:, None] == jnp.arange(row_blocks * row_count, dtype=jnp.int32)[None, :]) & live[:, None]
    stacked = jnp.stack([slot_ids, far_rank[0, 0]], axis=0)
    table = jnp.sum(jnp.where(match[None], stacked[:, :, None], 0), axis=1)
    table = table.reshape(2, row_blocks, row_count)
    bf16, f32 = jnp.bfloat16, jnp.float32
    any_space = pl.BlockSpec(memory_space=pl.ANY)
    smem = pl.BlockSpec(memory_space=pltpu.SMEM)
    vmem = pl.BlockSpec(memory_space=pltpu.VMEM)
    dma = pltpu.SemaphoreType.DMA
    return pl.pallas_call(
        functools.partial(fused_kernel, row_count // 4),
        out_shape=jax.ShapeDtypeStruct(incident.shape, bf16),
        in_specs=[smem, smem, vmem, any_space, any_space, any_space],
        out_specs=vmem,
        scratch_shapes=[
            pltpu.VMEM((waves, row_count + 2, tile_rows, columns), bf16),
            pltpu.VMEM((waves, near_slots, 2, tile_rows, tile_rows), bf16),
            pltpu.VMEM((waves, slots, 2, rank_rows, tile_rows), bf16),
            pltpu.VMEM((waves, slots, 2, rank_rows, tile_rows), bf16),
            pltpu.VMEM((waves, row_blocks, 2, row_count, rank_rows, tile_rows), bf16),
            pltpu.VMEM((waves, row_blocks, 2, row_count, rank_rows, columns), bf16),
            pltpu.VMEM((waves, tile_rows, columns), f32),
            pltpu.VMEM((waves, tile_rows, columns), f32),
            pltpu.VMEM((waves, tile_rows, columns), f32),
            dma((waves, row_count + 2)),
            dma((waves, row_count, 4)),
            dma((waves, 2)),
            dma((waves,)),
            dma((waves,)),
            dma((3,)),
        ],
        compiler_params=pltpu.CompilerParams(collective_id=0, has_side_effects=True),
    )(table, near_offsets[0], incident, near_tiles, far_u, far_v)


def solution(mesh):
    in_specs = (
        P(None, ("row", "col"), None),
        P(("row", "col"), None, None, None, None, None),
        P(("row", "col"), None),
        P("row", "col", None),
        P("row", "col", None),
        P("row", "col", None),
        P("row", "col"),
        P("row", "col", None, None, None, None, None),
        P("row", "col", None, None, None, None, None),
    )
    out_specs = P(None, ("row", "col"), None)
    paired = mesh.shape["col"] == 2 and mesh.shape["row"] % 4 == 0 and mesh.shape["row"] > 4
    shards = fused_shards if paired else generic_shards
    return jax.shard_map(shards, mesh=mesh, in_specs=in_specs, out_specs=out_specs, check_vma=False)
```

```python
import functools

import jax
import jax.numpy as jnp
from jax import lax
from jax.experimental import pallas as pl
from jax.experimental.pallas import tpu as pltpu
from jax.sharding import PartitionSpec as P

MESH = pl.DeviceIdType.MESH
UP, DOWN, ALONG_Y, ALONG_X = range(4)


def from_behind(value, axis, steps):
    count = lax.axis_size(axis)
    pairs = [(source, (source + steps) % count) for source in range(count)]
    return lax.ppermute(value, axis, pairs)


def combine_parts(real_prod, imag_prod):
    half_width = real_prod.shape[-1] // 2
    return jnp.concatenate(
        [
            real_prod[..., :half_width] - imag_prod[..., half_width:],
            real_prod[..., half_width:] + imag_prod[..., :half_width],
        ],
        axis=-1,
    )


def far_partial(
    wave_tiles,
    rows_local,
    cols_local,
    rank_local,
    live_count,
    u_wave,
    v_wave,
    group_limit,
    row_blocks,
):
    group_size = 16
    tile_rows = wave_tiles.shape[1]
    columns = wave_tiles.shape[2]
    rank_size = v_wave.shape[2]
    slot_ids = jnp.arange(group_size, dtype=jnp.int32)
    rank_ids = jnp.arange(rank_size, dtype=jnp.int32)

    def add_group(group_step, far_sum):
        first_slot = group_step * group_size
        rows_group = lax.dynamic_slice_in_dim(rows_local, first_slot, group_size)
        cols_group = lax.dynamic_slice_in_dim(cols_local, first_slot, group_size)
        rank_group = lax.dynamic_slice_in_dim(rank_local, first_slot, group_size)
        v_group = lax.dynamic_slice_in_dim(v_wave, first_slot, group_size, 0)
        u_group = lax.dynamic_slice_in_dim(u_wave, first_slot, group_size, 0)
        slot_tiles = jnp.take(wave_tiles, cols_group, axis=0)
        real_prod = jnp.einsum(
            "fkq,fqc->fkc", v_group[:, 0], slot_tiles, preferred_element_type=jnp.float32
        )
        imag_prod = jnp.einsum(
            "fkq,fqc->fkc", v_group[:, 1], slot_tiles, preferred_element_type=jnp.float32
        )
        live_mask = (first_slot + slot_ids < live_count)[:, None] & (
            rank_ids[None, :] < rank_group[:, None]
        )
        coefficients = (
            combine_parts(real_prod, imag_prod) * live_mask[:, :, None].astype(jnp.float32)
        ).astype(jnp.bfloat16)
        real_back = jnp.einsum(
            "fkp,fkc->fpc", u_group[:, 0], coefficients, preferred_element_type=jnp.float32
        )
        imag_back = jnp.einsum(
            "fkp,fkc->fpc", u_group[:, 1], coefficients, preferred_element_type=jnp.float32
        )
        contrib = combine_parts(real_back, imag_back)
        return far_sum.at[rows_group].add(contrib)

    zero_sum = jnp.zeros((row_blocks, tile_rows, columns), jnp.float32)
    return lax.fori_loop(0, group_limit, add_group, zero_sum)


def reduce_rows(far_sum, row_blocks, tile_rows, columns):
    flat_rows = far_sum.reshape(row_blocks * tile_rows, columns)
    return lax.psum_scatter(flat_rows, "col", scatter_dimension=0, tiled=True)


def generic_shards(incident, near_tiles, near_offsets, far_row, far_col, far_rank, far_count, far_u, far_v):
    wave_count, tile_rows, columns = incident.shape
    row_blocks = lax.axis_size("col")
    slot_count = far_row.shape[2]
    stacked = []
    for shift_by in (2, 1, 0, -1, -2):
        if shift_by == 0:
            stacked.append(incident)
        else:
            stacked.append(from_behind(incident, ("row", "col"), shift_by))
    neighbour = jnp.stack(stacked, axis=1)
    near_inputs = jnp.take(neighbour, near_offsets[0] + 2, axis=1)
    local_near = near_tiles[0]
    real_prod = jnp.einsum(
        "wnpq,wnqc->wpc", local_near[:, :, 0], near_inputs, preferred_element_type=jnp.float32
    )
    imag_prod = jnp.einsum(
        "wnpq,wnqc->wpc", local_near[:, :, 1], near_inputs, preferred_element_type=jnp.float32
    )
    near_total = combine_parts(real_prod, imag_prod)
    rows_local = far_row[0, 0]
    cols_local = far_col[0, 0]
    rank_local = far_rank[0, 0]
    live_count = far_count[0, 0]
    group_limit = slot_count // 16
    gathered = lax.all_gather(incident, "row", axis=1, tiled=True)
    outputs = []
    for wave_index in range(wave_count):
        wave_columns = gathered[wave_index]
        wave_tiles = wave_columns.reshape(-1, tile_rows, columns)
        far_sum = far_partial(
            wave_tiles,
            rows_local,
            cols_local,
            rank_local,
            live_count,
            far_u[0, 0, wave_index],
            far_v[0, 0, wave_index],
            group_limit,
            row_blocks,
        )
        own_rows = reduce_rows(far_sum, row_blocks, tile_rows, columns)
        outputs.append(near_total[wave_index] + own_rows)
    return jnp.stack(outputs, axis=0).astype(jnp.bfloat16)


def turned(block):
    half = block.shape[-1] // 2
    return jnp.concatenate([-block[:, half:], block[:, :half]], axis=-1)


def fused_kernel(
    depth, slot_ref, offset_ref, x_ref, near_hbm, u_hbm, v_hbm, out_ref,
    tiles, near_buf, u_buf, v_buf, u_dense, coef, v_out, v_in, coef_out, outgoing, incoming, total,
    recv_sem, send_sem, pair_sem, v_send, v_recv, c_send, c_recv, sum_send, sum_recv, load_sem,
):
    waves = x_ref.shape[0]
    row_count = depth * 4
    row_blocks = slot_ref.shape[1]
    rank_rows = v_buf.shape[3]
    r = lax.axis_index("row")
    c = lax.axis_index("col")
    z, y, x = r // 4, (r // 2) % 2, r % 2
    own_slot, edge_slot = row_count, row_count + 1
    edge_tile = (r + 1 - 2 * c + row_count) % row_count
    side = 2 * x - 1
    partner = r + 2 * (1 - 2 * y)
    corner = (r + side + row_count) % row_count
    partner_corner = (partner + side + row_count) % row_count

    def row_of(tz, ty, tx):
        return (tz * 2 + ty) * 2 + tx

    loads = [
        pltpu.make_async_copy(v_hbm.at[0, 0], v_buf, load_sem.at[0]),
        pltpu.make_async_copy(u_hbm.at[0, 0], u_buf, load_sem.at[1]),
        pltpu.make_async_copy(near_hbm.at[0], near_buf, load_sem.at[2]),
    ]
    for load in loads:
        load.start()

    barrier = pltpu.get_barrier_semaphore()
    greeted = (
        (row_of((z + 1) % depth, y, x), c),
        (row_of((z + depth - 1) % depth, y, x), c),
        (partner, c),
        (row_of(z, y, 1 - x), c),
        (r, 1 - c),
    )
    for device in greeted:
        pl.semaphore_signal(barrier, inc=1, device_id=device, device_id_type=MESH)
    pl.semaphore_wait(barrier, len(greeted))

    def copy_to(source, target, sent, received, device):
        return pltpu.make_async_remote_copy(
            src_ref=source,
            dst_ref=target,
            send_sem=sent,
            recv_sem=received,
            device_id=device,
            device_id_type=MESH,
        )

    def hop(wave, tile, link, row, source=None):
        here = tiles.at[wave, tile]
        return copy_to(
            here if source is None else source,
            here,
            send_sem.at[wave, tile, link],
            recv_sem.at[wave, tile],
            (row, c),
        )

    def along_z(wave, tile, step, source=None):
        target = jnp.minimum(jnp.maximum(z + step, 0), depth - 1)
        return hop(wave, tile, (1 - step) // 2, row_of(target, y, x), source)

    def along_x(wave, tile, source=None):
        return hop(wave, tile, ALONG_X, row_of(z, y, 1 - x), source)

    def along_y(wave, tile, source=None):
        return hop(wave, tile, ALONG_Y, partner, source)

    def to_pair(wave, source, slot):
        return copy_to(
            source,
            tiles.at[wave, slot],
            pair_sem.at[wave, slot - row_count],
            recv_sem.at[wave, slot],
            (r, 1 - c),
        )

    def send_v(place):
        return copy_to(
            v_out.at[place], v_in.at[place], v_send.at[place], v_recv.at[place], (partner, c)
        )

    def send_coef(place, tile):
        return copy_to(
            coef_out.at[place], coef.at[0, tile], c_send.at[place], c_recv.at[place], (partner, c)
        )

    rank_ids = lax.broadcasted_iota(jnp.int32, (rank_rows, v_buf.shape[4]), 0)

    def complex_rows(prod, a):
        at = 2 * rank_rows * a
        return combine_parts(prod[at:at + rank_rows], prod[at + rank_rows:at + 2 * rank_rows])

    def project(wave, tile):
        block = tiles[wave, tile]
        factors = [
            v_buf[wave, slot_ref[0, a, tile]].reshape(2 * rank_rows, -1) for a in range(row_blocks)
        ]
        prod = jnp.dot(
            jnp.concatenate(factors, axis=0), block, preferred_element_type=jnp.float32
        )
        ids = lax.broadcasted_iota(jnp.int32, (rank_rows, block.shape[1]), 0)
        for a in range(row_blocks):
            both = jnp.where(ids < slot_ref[1, a, tile], complex_rows(prod, a), 0.0)
            coef[0, tile, wave, a] = both.astype(jnp.bfloat16)
            coef[1, tile, wave, a] = turned(both).astype(jnp.bfloat16)

    def serve(place, tile):
        for wave in range(waves):
            left = v_in[place, wave].reshape(row_blocks * 2 * rank_rows, -1)
            prod = jnp.dot(left, tiles[wave, tile], preferred_element_type=jnp.float32)
            for a in range(row_blocks):
                coef_out[place, wave, a] = complex_rows(prod, a).astype(jnp.bfloat16)

    def use_tile(level, tx):
        tile, place = row_of(level, y, tx), level * 2 + tx

        @pl.when(tile == partner_corner)
        def _():
            for wave in range(waves):
                along_y(wave, tile).start()

        @pl.when(tile != partner_corner)
        def _():
            send_v(place).wait_recv()
            serve(place, tile)

        for wave in range(waves):
            project(wave, tile)

        @pl.when(tile != partner_corner)
        def _():
            send_coef(place, tile).start()

    def arrive(wave, tile):
        pltpu.make_async_copy(tiles.at[wave, tile], tiles.at[wave, tile], recv_sem.at[wave, tile]).wait()

    def share_edge(wave, tile):
        @pl.when(tile == edge_tile)
        def _():
            to_pair(wave, tiles.at[wave, tile], edge_slot).start()

    level_count = 2 * depth - 1
    lag = 2

    def level_of(step):
        sign = 1 - 2 * (step % 2)
        return z + sign * ((step + 1) // 2), sign

    def inside(level):
        return (level >= 0) & (level < depth)

    for wave in range(waves):
        own = x_ref.at[wave]
        along_x(wave, r, own).start()

        @pl.when(z < depth - 1)
        def _():
            along_z(wave, r, 1, own).start()

        @pl.when(z > 0)
        def _():
            along_z(wave, r, -1, own).start()

        to_pair(wave, own, own_slot).start()
        tiles[wave, r] = x_ref[wave]

    loads[0].wait()

    def place_v(place, carry):
        tile = row_of(place // 2, 1 - y, place % 2)
        for wave in range(waves):
            for a in range(row_blocks):
                factor = v_buf[wave, slot_ref[0, a, tile]]
                for part in range(2):
                    kept = factor[part].astype(jnp.float32)
                    kept = jnp.where(rank_ids < slot_ref[1, a, tile], kept, 0.0)
                    v_out[place, wave, a, part] = kept.astype(jnp.bfloat16)
        return carry

    lax.fori_loop(0, 2 * depth, place_v, 0)

    def push_v(step, carry):
        level, _ = level_of(step // 2)
        tx = (x + step) % 2

        @pl.when(inside(level) & (row_of(level, 1 - y, tx) != corner))
        def _():
            send_v(level * 2 + tx).start()

        return carry

    lax.fori_loop(0, 2 * level_count, push_v, 0)

    for load in loads[1:]:
        load.wait()

    def place_u(tile, carry):
        for wave in range(waves):
            for a in range(row_blocks):
                factor = u_buf[wave, slot_ref[0, a, tile]]
                u_dense[wave, a, 0, tile] = factor[0]
                u_dense[wave, a, 1, tile] = factor[1]
        return carry

    lax.fori_loop(0, row_count, place_u, 0)

    def spread(step, carry):
        level, sign = level_of(step)

        @pl.when((step < level_count) & inside(level))
        def _():
            tile = row_of(level, y, x)

            @pl.when(step > 0)
            def _():
                for wave in range(waves):
                    arrive(wave, tile)

                    @pl.when(inside(z - sign))
                    def _():
                        along_z(wave, tile, -sign).start()

                    along_x(wave, tile).start()

            use_tile(level, x)

        behind, _ = level_of(jnp.maximum(step - lag, 0))

        @pl.when((step >= lag) & inside(behind))
        def _():
            tile = row_of(behind, y, 1 - x)
            for wave in range(waves):
                arrive(wave, tile)
                share_edge(wave, tile)
            use_tile(behind, 1 - x)

        return carry

    lax.fori_loop(0, level_count + lag, spread, 0)

    for wave in range(waves):
        arrive(wave, corner)
        share_edge(wave, corner)
        project(wave, corner)

    def finish(place, carry):
        tile = row_of(place // 2, 1 - y, place % 2)

        @pl.when(tile != corner)
        def _():
            send_coef(place, tile).wait_recv()
            for wave in range(waves):
                for a in range(row_blocks):
                    coef[1, tile, wave, a] = turned(coef[0, tile, wave, a])

        return carry

    lax.fori_loop(0, 2 * depth, finish, 0)

    def far_sum(wave, a):
        left = u_dense[wave, a].reshape(-1, u_dense.shape[-1])
        right = coef[:, :, wave, a].reshape(-1, coef.shape[-1])
        return lax.dot_general(
            left, right, (((0,), (0,)), ((), ())), preferred_element_type=jnp.float32
        )

    def send_sum(wave):
        return copy_to(
            outgoing.at[wave], incoming.at[wave], sum_send.at[wave], sum_recv.at[wave], (r, 1 - c)
        )

    def fill(wave, carry):
        outgoing[wave] = far_sum(wave, 1 - c)
        return carry

    lax.fori_loop(0, waves, fill, 0)
    for wave in range(waves):
        arrive(wave, own_slot)
        arrive(wave, edge_slot)

    def place_of(offset):
        even = (r + offset // 2 + row_count) % row_count
        same_chip = offset == 1 - 2 * c
        return jnp.where(offset % 2 == 0, even, jnp.where(same_chip, own_slot, edge_slot))

    def own_rows(wave, carry):
        send_sum(wave).start()
        value = far_sum(wave, c)
        for n in range(near_buf.shape[1]):
            block = tiles[wave, place_of(offset_ref[n])]
            value += jnp.dot(near_buf[wave, n, 0], block, preferred_element_type=jnp.float32)
            value += jnp.dot(
                near_buf[wave, n, 1], turned(block), preferred_element_type=jnp.float32
            )
        total[wave] = value
        return carry

    lax.fori_loop(0, waves, own_rows, 0)
    for wave in range(waves):
        send_sum(wave).wait()
        out_ref[wave] = (total[wave] + incoming[wave]).astype(out_ref.dtype)

    for wave in range(waves):
        to_pair(wave, x_ref.at[wave], own_slot).wait_send()
        to_pair(wave, x_ref.at[wave], edge_slot).wait_send()
        along_y(wave, partner_corner).wait_send()

    def drain(level, carry):
        tile = row_of(level, y, x)
        for wave in range(waves):
            along_x(wave, tile).wait_send()

            @pl.when((level <= z) & (z < depth - 1))
            def _():
                along_z(wave, tile, 1).wait_send()

            @pl.when((level >= z) & (z > 0))
            def _():
                along_z(wave, tile, -1).wait_send()

        for tx in range(2):
            place = level * 2 + tx

            @pl.when(row_of(level, 1 - y, tx) != corner)
            def _():
                send_v(place).wait_send()

            @pl.when(row_of(level, y, tx) != partner_corner)
            def _():
                send_coef(place, row_of(level, y, tx)).wait_send()
        return carry

    lax.fori_loop(0, depth, drain, 0)


def fused_shards(incident, near_tiles, near_offsets, far_row, far_col, far_rank, far_count, far_u, far_v):
    waves, tile_rows, columns = incident.shape
    row_count, row_blocks = lax.axis_size("row"), lax.axis_size("col")
    slots, rank_rows = far_u.shape[3], far_u.shape[5]
    near_slots = near_tiles.shape[2]
    slot_ids = jnp.arange(slots, dtype=jnp.int32)
    block_key = far_row[0, 0] * row_count + far_col[0, 0]
    live = slot_ids < far_count[0, 0]
    match = (block_key[:, None] == jnp.arange(row_blocks * row_count, dtype=jnp.int32)[None, :]) & live[:, None]
    stacked = jnp.stack([slot_ids, far_rank[0, 0]], axis=0)
    table = jnp.sum(jnp.where(match[None], stacked[:, :, None], 0), axis=1)
    table = table.reshape(2, row_blocks, row_count)
    bf16, f32 = jnp.bfloat16, jnp.float32
    any_space = pl.BlockSpec(memory_space=pl.ANY)
    smem = pl.BlockSpec(memory_space=pltpu.SMEM)
    vmem = pl.BlockSpec(memory_space=pltpu.VMEM)
    dma = pltpu.SemaphoreType.DMA
    return pl.pallas_call(
        functools.partial(fused_kernel, row_count // 4),
        out_shape=jax.ShapeDtypeStruct(incident.shape, bf16),
        in_specs=[smem, smem, vmem, any_space, any_space, any_space],
        out_specs=vmem,
        scratch_shapes=[
            pltpu.VMEM((waves, row_count + 2, tile_rows, columns), bf16),
            pltpu.VMEM((waves, near_slots, 2, tile_rows, tile_rows), bf16),
            pltpu.VMEM((waves, slots, 2, rank_rows, tile_rows), bf16),
            pltpu.VMEM((waves, slots, 2, rank_rows, tile_rows), bf16),
            pltpu.VMEM((waves, row_blocks, 2, row_count, rank_rows, tile_rows), bf16),
            pltpu.VMEM((2, row_count, waves, row_blocks, rank_rows, columns), bf16),
            pltpu.VMEM((row_count // 2, waves, row_blocks, 2, rank_rows, tile_rows), bf16),
            pltpu.VMEM((row_count // 2, waves, row_blocks, 2, rank_rows, tile_rows), bf16),
            pltpu.VMEM((row_count // 2, waves, row_blocks, rank_rows, columns), bf16),
            pltpu.VMEM((waves, tile_rows, columns), f32),
            pltpu.VMEM((waves, tile_rows, columns), f32),
            pltpu.VMEM((waves, tile_rows, columns), f32),
            dma((waves, row_count + 2)),
            dma((waves, row_count, 4)),
            dma((waves, 2)),
            dma((row_count // 2,)),
            dma((row_count // 2,)),
            dma((row_count // 2,)),
            dma((row_count // 2,)),
            dma((waves,)),
            dma((waves,)),
            dma((3,)),
        ],
        compiler_params=pltpu.CompilerParams(collective_id=0, has_side_effects=True),
    )(table, near_offsets[0], incident, near_tiles, far_u, far_v)


def solution(mesh):
    in_specs = (
        P(None, ("row", "col"), None),
        P(("row", "col"), None, None, None, None, None),
        P(("row", "col"), None),
        P("row", "col", None),
        P("row", "col", None),
        P("row", "col", None),
        P("row", "col"),
        P("row", "col", None, None, None, None, None),
        P("row", "col", None, None, None, None, None),
    )
    out_specs = P(None, ("row", "col"), None)
    paired = mesh.shape["col"] == 2 and mesh.shape["row"] % 4 == 0 and mesh.shape["row"] > 4
    shards = fused_shards if paired else generic_shards
    return jax.shard_map(shards, mesh=mesh, in_specs=in_specs, out_specs=out_specs, check_vma=False)
```

```python
import functools

import jax
import jax.numpy as jnp
from jax import lax
from jax.experimental import pallas as pl
from jax.experimental.pallas import tpu as pltpu
from jax.sharding import PartitionSpec as P

MESH = pl.DeviceIdType.MESH
UP, DOWN, ALONG_Y, ALONG_X = range(4)


def from_behind(value, axis, steps):
    count = lax.axis_size(axis)
    pairs = [(source, (source + steps) % count) for source in range(count)]
    return lax.ppermute(value, axis, pairs)


def combine_parts(real_prod, imag_prod):
    half_width = real_prod.shape[-1] // 2
    return jnp.concatenate(
        [
            real_prod[..., :half_width] - imag_prod[..., half_width:],
            real_prod[..., half_width:] + imag_prod[..., :half_width],
        ],
        axis=-1,
    )


def far_partial(
    wave_tiles,
    rows_local,
    cols_local,
    rank_local,
    live_count,
    u_wave,
    v_wave,
    group_limit,
    row_blocks,
):
    group_size = 16
    tile_rows = wave_tiles.shape[1]
    columns = wave_tiles.shape[2]
    rank_size = v_wave.shape[2]
    slot_ids = jnp.arange(group_size, dtype=jnp.int32)
    rank_ids = jnp.arange(rank_size, dtype=jnp.int32)

    def add_group(group_step, far_sum):
        first_slot = group_step * group_size
        rows_group = lax.dynamic_slice_in_dim(rows_local, first_slot, group_size)
        cols_group = lax.dynamic_slice_in_dim(cols_local, first_slot, group_size)
        rank_group = lax.dynamic_slice_in_dim(rank_local, first_slot, group_size)
        v_group = lax.dynamic_slice_in_dim(v_wave, first_slot, group_size, 0)
        u_group = lax.dynamic_slice_in_dim(u_wave, first_slot, group_size, 0)
        slot_tiles = jnp.take(wave_tiles, cols_group, axis=0)
        real_prod = jnp.einsum(
            "fkq,fqc->fkc", v_group[:, 0], slot_tiles, preferred_element_type=jnp.float32
        )
        imag_prod = jnp.einsum(
            "fkq,fqc->fkc", v_group[:, 1], slot_tiles, preferred_element_type=jnp.float32
        )
        live_mask = (first_slot + slot_ids < live_count)[:, None] & (
            rank_ids[None, :] < rank_group[:, None]
        )
        coefficients = (
            combine_parts(real_prod, imag_prod) * live_mask[:, :, None].astype(jnp.float32)
        ).astype(jnp.bfloat16)
        real_back = jnp.einsum(
            "fkp,fkc->fpc", u_group[:, 0], coefficients, preferred_element_type=jnp.float32
        )
        imag_back = jnp.einsum(
            "fkp,fkc->fpc", u_group[:, 1], coefficients, preferred_element_type=jnp.float32
        )
        contrib = combine_parts(real_back, imag_back)
        return far_sum.at[rows_group].add(contrib)

    zero_sum = jnp.zeros((row_blocks, tile_rows, columns), jnp.float32)
    return lax.fori_loop(0, group_limit, add_group, zero_sum)


def reduce_rows(far_sum, row_blocks, tile_rows, columns):
    flat_rows = far_sum.reshape(row_blocks * tile_rows, columns)
    return lax.psum_scatter(flat_rows, "col", scatter_dimension=0, tiled=True)


def generic_shards(incident, near_tiles, near_offsets, far_row, far_col, far_rank, far_count, far_u, far_v):
    wave_count, tile_rows, columns = incident.shape
    row_blocks = lax.axis_size("col")
    slot_count = far_row.shape[2]
    stacked = []
    for shift_by in (2, 1, 0, -1, -2):
        if shift_by == 0:
            stacked.append(incident)
        else:
            stacked.append(from_behind(incident, ("row", "col"), shift_by))
    neighbour = jnp.stack(stacked, axis=1)
    near_inputs = jnp.take(neighbour, near_offsets[0] + 2, axis=1)
    local_near = near_tiles[0]
    real_prod = jnp.einsum(
        "wnpq,wnqc->wpc", local_near[:, :, 0], near_inputs, preferred_element_type=jnp.float32
    )
    imag_prod = jnp.einsum(
        "wnpq,wnqc->wpc", local_near[:, :, 1], near_inputs, preferred_element_type=jnp.float32
    )
    near_total = combine_parts(real_prod, imag_prod)
    rows_local = far_row[0, 0]
    cols_local = far_col[0, 0]
    rank_local = far_rank[0, 0]
    live_count = far_count[0, 0]
    group_limit = slot_count // 16
    gathered = lax.all_gather(incident, "row", axis=1, tiled=True)
    outputs = []
    for wave_index in range(wave_count):
        wave_columns = gathered[wave_index]
        wave_tiles = wave_columns.reshape(-1, tile_rows, columns)
        far_sum = far_partial(
            wave_tiles,
            rows_local,
            cols_local,
            rank_local,
            live_count,
            far_u[0, 0, wave_index],
            far_v[0, 0, wave_index],
            group_limit,
            row_blocks,
        )
        own_rows = reduce_rows(far_sum, row_blocks, tile_rows, columns)
        outputs.append(near_total[wave_index] + own_rows)
    return jnp.stack(outputs, axis=0).astype(jnp.bfloat16)


def turned(block):
    half = block.shape[-1] // 2
    return jnp.concatenate([-block[:, half:], block[:, :half]], axis=-1)


def fused_kernel(
    depth, slot_ref, offset_ref, x_ref, near_hbm, u_hbm, v_hbm, out_ref,
    tiles, near_buf, u_buf, v_buf, u_dense, coef, v_out, v_in, coef_out, outgoing, incoming, total,
    recv_sem, send_sem, pair_sem, v_send, v_recv, c_send, c_recv, sum_send, sum_recv, load_sem,
):
    waves = x_ref.shape[0]
    row_count = depth * 4
    row_blocks = slot_ref.shape[1]
    rank_rows = v_buf.shape[3]
    r = lax.axis_index("row")
    c = lax.axis_index("col")
    z, y, x = r // 4, (r // 2) % 2, r % 2
    own_slot, edge_slot = row_count, row_count + 1
    edge_tile = (r + 1 - 2 * c + row_count) % row_count
    side = 2 * x - 1
    partner = r + 2 * (1 - 2 * y)
    corner = (r + side + row_count) % row_count
    partner_corner = (partner + side + row_count) % row_count

    def row_of(tz, ty, tx):
        return (tz * 2 + ty) * 2 + tx

    loads = [
        pltpu.make_async_copy(v_hbm.at[0, 0], v_buf, load_sem.at[0]),
        pltpu.make_async_copy(u_hbm.at[0, 0], u_buf, load_sem.at[1]),
        pltpu.make_async_copy(near_hbm.at[0], near_buf, load_sem.at[2]),
    ]
    for load in loads:
        load.start()

    barrier = pltpu.get_barrier_semaphore()
    greeted = (
        (row_of((z + 1) % depth, y, x), c),
        (row_of((z + depth - 1) % depth, y, x), c),
        (partner, c),
        (row_of(z, y, 1 - x), c),
        (r, 1 - c),
    )
    for device in greeted:
        pl.semaphore_signal(barrier, inc=1, device_id=device, device_id_type=MESH)
    pl.semaphore_wait(barrier, len(greeted))

    def copy_to(source, target, sent, received, device):
        return pltpu.make_async_remote_copy(
            src_ref=source,
            dst_ref=target,
            send_sem=sent,
            recv_sem=received,
            device_id=device,
            device_id_type=MESH,
        )

    def hop(wave, tile, link, row, source=None):
        here = tiles.at[wave, tile]
        return copy_to(
            here if source is None else source,
            here,
            send_sem.at[wave, tile, link],
            recv_sem.at[wave, tile],
            (row, c),
        )

    def along_z(wave, tile, step, source=None):
        target = (z + step + depth) % depth
        return hop(wave, tile, (1 - step) // 2, row_of(target, y, x), source)

    def along_x(wave, tile, source=None):
        return hop(wave, tile, ALONG_X, row_of(z, y, 1 - x), source)

    def along_y(wave, tile, source=None):
        return hop(wave, tile, ALONG_Y, partner, source)

    def to_pair(wave, source, slot):
        return copy_to(
            source,
            tiles.at[wave, slot],
            pair_sem.at[wave, slot - row_count],
            recv_sem.at[wave, slot],
            (r, 1 - c),
        )

    def send_v(place):
        return copy_to(
            v_out.at[place], v_in.at[place], v_send.at[place], v_recv.at[place], (partner, c)
        )

    def send_coef(place, tile):
        return copy_to(
            coef_out.at[place], coef.at[0, tile], c_send.at[place], c_recv.at[place], (partner, c)
        )

    rank_ids = lax.broadcasted_iota(jnp.int32, (rank_rows, v_buf.shape[4]), 0)

    def complex_rows(prod, a):
        at = 2 * rank_rows * a
        return combine_parts(prod[at:at + rank_rows], prod[at + rank_rows:at + 2 * rank_rows])

    def project(wave, tile):
        block = tiles[wave, tile]
        factors = [
            v_buf[wave, slot_ref[0, a, tile]].reshape(2 * rank_rows, -1) for a in range(row_blocks)
        ]
        prod = jnp.dot(
            jnp.concatenate(factors, axis=0), block, preferred_element_type=jnp.float32
        )
        ids = lax.broadcasted_iota(jnp.int32, (rank_rows, block.shape[1]), 0)
        for a in range(row_blocks):
            both = jnp.where(ids < slot_ref[1, a, tile], complex_rows(prod, a), 0.0)
            coef[0, tile, wave, a] = both.astype(jnp.bfloat16)
            coef[1, tile, wave, a] = turned(both).astype(jnp.bfloat16)

    def serve(place, tile):
        for wave in range(waves):
            left = v_in[place, wave].reshape(row_blocks * 2 * rank_rows, -1)
            prod = jnp.dot(left, tiles[wave, tile], preferred_element_type=jnp.float32)
            for a in range(row_blocks):
                coef_out[place, wave, a] = complex_rows(prod, a).astype(jnp.bfloat16)

    def use_tile(level, tx):
        tile, place = row_of(level, y, tx), level * 2 + tx

        @pl.when(tile == partner_corner)
        def _():
            for wave in range(waves):
                along_y(wave, tile).start()

        @pl.when(tile != partner_corner)
        def _():
            send_v(place).wait_recv()
            serve(place, tile)

        for wave in range(waves):
            project(wave, tile)

        @pl.when(tile != partner_corner)
        def _():
            send_coef(place, tile).start()

    def arrive(wave, tile):
        pltpu.make_async_copy(tiles.at[wave, tile], tiles.at[wave, tile], recv_sem.at[wave, tile]).wait()

    def share_edge(wave, tile):
        @pl.when(tile == edge_tile)
        def _():
            to_pair(wave, tiles.at[wave, tile], edge_slot).start()

    lag = 2

    def level_of(step):
        sign = 1 - 2 * (step % 2)
        return (z + sign * ((step + 1) // 2) + depth) % depth, sign

    def reach(wave, step):
        return depth // 2 if (step == 1) == (wave % 2 == 0) else (depth - 1) // 2

    for wave in range(waves):
        own = x_ref.at[wave]
        along_x(wave, r, own).start()
        for step in (1, -1):
            if reach(wave, step) > 0:
                along_z(wave, r, step, own).start()
        to_pair(wave, own, own_slot).start()
        tiles[wave, r] = x_ref[wave]

    loads[0].wait()

    def place_v(place, carry):
        tile = row_of(place // 2, 1 - y, place % 2)
        for wave in range(waves):
            for a in range(row_blocks):
                factor = v_buf[wave, slot_ref[0, a, tile]]
                for part in range(2):
                    kept = factor[part].astype(jnp.float32)
                    kept = jnp.where(rank_ids < slot_ref[1, a, tile], kept, 0.0)
                    v_out[place, wave, a, part] = kept.astype(jnp.bfloat16)
        return carry

    lax.fori_loop(0, 2 * depth, place_v, 0)

    def push_v(step, carry):
        level, _ = level_of(step // 2)
        tx = (x + step) % 2

        @pl.when(row_of(level, 1 - y, tx) != corner)
        def _():
            send_v(level * 2 + tx).start()

        return carry

    lax.fori_loop(0, 2 * depth, push_v, 0)

    for load in loads[1:]:
        load.wait()

    def place_u(tile, carry):
        for wave in range(waves):
            for a in range(row_blocks):
                factor = u_buf[wave, slot_ref[0, a, tile]]
                u_dense[wave, a, 0, tile] = factor[0]
                u_dense[wave, a, 1, tile] = factor[1]
        return carry

    lax.fori_loop(0, row_count, place_u, 0)

    def spread(step, carry):
        level, sign = level_of(step)

        @pl.when(step < depth)
        def _():
            tile = row_of(level, y, x)

            @pl.when(step > 0)
            def _():
                for wave in range(waves):
                    arrive(wave, tile)

                    for move in (1, -1):
                        @pl.when((sign == -move) & ((step + 1) // 2 < reach(wave, move)))
                        def _():
                            along_z(wave, tile, move).start()

                    along_x(wave, tile).start()

            use_tile(level, x)

        behind, _ = level_of(jnp.maximum(step - lag, 0))

        @pl.when(step >= lag)
        def _():
            tile = row_of(behind, y, 1 - x)
            for wave in range(waves):
                arrive(wave, tile)
                share_edge(wave, tile)
            use_tile(behind, 1 - x)

        return carry

    lax.fori_loop(0, depth + lag, spread, 0)

    for wave in range(waves):
        arrive(wave, corner)
        share_edge(wave, corner)
        project(wave, corner)

    def finish(place, carry):
        tile = row_of(place // 2, 1 - y, place % 2)

        @pl.when(tile != corner)
        def _():
            send_coef(place, tile).wait_recv()
            for wave in range(waves):
                for a in range(row_blocks):
                    coef[1, tile, wave, a] = turned(coef[0, tile, wave, a])

        return carry

    lax.fori_loop(0, 2 * depth, finish, 0)

    def far_sum(wave, a):
        left = u_dense[wave, a].reshape(-1, u_dense.shape[-1])
        right = coef[:, :, wave, a].reshape(-1, coef.shape[-1])
        return lax.dot_general(
            left, right, (((0,), (0,)), ((), ())), preferred_element_type=jnp.float32
        )

    def send_sum(wave):
        return copy_to(
            outgoing.at[wave], incoming.at[wave], sum_send.at[wave], sum_recv.at[wave], (r, 1 - c)
        )

    def fill(wave, carry):
        outgoing[wave] = far_sum(wave, 1 - c)
        return carry

    lax.fori_loop(0, waves, fill, 0)
    for wave in range(waves):
        arrive(wave, own_slot)
        arrive(wave, edge_slot)

    def place_of(offset):
        even = (r + offset // 2 + row_count) % row_count
        same_chip = offset == 1 - 2 * c
        return jnp.where(offset % 2 == 0, even, jnp.where(same_chip, own_slot, edge_slot))

    def own_rows(wave, carry):
        send_sum(wave).start()
        value = far_sum(wave, c)
        for n in range(near_buf.shape[1]):
            block = tiles[wave, place_of(offset_ref[n])]
            value += jnp.dot(near_buf[wave, n, 0], block, preferred_element_type=jnp.float32)
            value += jnp.dot(
                near_buf[wave, n, 1], turned(block), preferred_element_type=jnp.float32
            )
        total[wave] = value
        return carry

    lax.fori_loop(0, waves, own_rows, 0)
    for wave in range(waves):
        send_sum(wave).wait()
        out_ref[wave] = (total[wave] + incoming[wave]).astype(out_ref.dtype)

    for wave in range(waves):
        to_pair(wave, x_ref.at[wave], own_slot).wait_send()
        to_pair(wave, x_ref.at[wave], edge_slot).wait_send()
        along_y(wave, partner_corner).wait_send()

    def drain(level, carry):
        tile = row_of(level, y, x)
        for wave in range(waves):
            along_x(wave, tile).wait_send()
            for move in (1, -1):
                @pl.when((move * (z - level) + depth) % depth < reach(wave, move))
                def _():
                    along_z(wave, tile, move).wait_send()

        for tx in range(2):
            place = level * 2 + tx

            @pl.when(row_of(level, 1 - y, tx) != corner)
            def _():
                send_v(place).wait_send()

            @pl.when(row_of(level, y, tx) != partner_corner)
            def _():
                send_coef(place, row_of(level, y, tx)).wait_send()
        return carry

    lax.fori_loop(0, depth, drain, 0)


def fused_shards(incident, near_tiles, near_offsets, far_row, far_col, far_rank, far_count, far_u, far_v):
    waves, tile_rows, columns = incident.shape
    row_count, row_blocks = lax.axis_size("row"), lax.axis_size("col")
    slots, rank_rows = far_u.shape[3], far_u.shape[5]
    near_slots = near_tiles.shape[2]
    slot_ids = jnp.arange(slots, dtype=jnp.int32)
    block_key = far_row[0, 0] * row_count + far_col[0, 0]
    live = slot_ids < far_count[0, 0]
    match = (block_key[:, None] == jnp.arange(row_blocks * row_count, dtype=jnp.int32)[None, :]) & live[:, None]
    stacked = jnp.stack([slot_ids, far_rank[0, 0]], axis=0)
    table = jnp.sum(jnp.where(match[None], stacked[:, :, None], 0), axis=1)
    table = table.reshape(2, row_blocks, row_count)
    bf16, f32 = jnp.bfloat16, jnp.float32
    any_space = pl.BlockSpec(memory_space=pl.ANY)
    smem = pl.BlockSpec(memory_space=pltpu.SMEM)
    vmem = pl.BlockSpec(memory_space=pltpu.VMEM)
    dma = pltpu.SemaphoreType.DMA
    return pl.pallas_call(
        functools.partial(fused_kernel, row_count // 4),
        out_shape=jax.ShapeDtypeStruct(incident.shape, bf16),
        in_specs=[smem, smem, vmem, any_space, any_space, any_space],
        out_specs=vmem,
        scratch_shapes=[
            pltpu.VMEM((waves, row_count + 2, tile_rows, columns), bf16),
            pltpu.VMEM((waves, near_slots, 2, tile_rows, tile_rows), bf16),
            pltpu.VMEM((waves, slots, 2, rank_rows, tile_rows), bf16),
            pltpu.VMEM((waves, slots, 2, rank_rows, tile_rows), bf16),
            pltpu.VMEM((waves, row_blocks, 2, row_count, rank_rows, tile_rows), bf16),
            pltpu.VMEM((2, row_count, waves, row_blocks, rank_rows, columns), bf16),
            pltpu.VMEM((row_count // 2, waves, row_blocks, 2, rank_rows, tile_rows), bf16),
            pltpu.VMEM((row_count // 2, waves, row_blocks, 2, rank_rows, tile_rows), bf16),
            pltpu.VMEM((row_count // 2, waves, row_blocks, rank_rows, columns), bf16),
            pltpu.VMEM((waves, tile_rows, columns), f32),
            pltpu.VMEM((waves, tile_rows, columns), f32),
            pltpu.VMEM((waves, tile_rows, columns), f32),
            dma((waves, row_count + 2)),
            dma((waves, row_count, 4)),
            dma((waves, 2)),
            dma((row_count // 2,)),
            dma((row_count // 2,)),
            dma((row_count // 2,)),
            dma((row_count // 2,)),
            dma((waves,)),
            dma((waves,)),
            dma((3,)),
        ],
        compiler_params=pltpu.CompilerParams(collective_id=0, has_side_effects=True),
    )(table, near_offsets[0], incident, near_tiles, far_u, far_v)


def solution(mesh):
    in_specs = (
        P(None, ("row", "col"), None),
        P(("row", "col"), None, None, None, None, None),
        P(("row", "col"), None),
        P("row", "col", None),
        P("row", "col", None),
        P("row", "col", None),
        P("row", "col"),
        P("row", "col", None, None, None, None, None),
        P("row", "col", None, None, None, None, None),
    )
    out_specs = P(None, ("row", "col"), None)
    paired = mesh.shape["col"] == 2 and mesh.shape["row"] % 4 == 0 and mesh.shape["row"] > 4
    shards = fused_shards if paired else generic_shards
    return jax.shard_map(shards, mesh=mesh, in_specs=in_specs, out_specs=out_specs, check_vma=False)
```
